512 devices in a mesh: row: 4 (over x), col: 4 (over z_lo), depth: 32 (over y, z_hi, core).
Axes of the slice: x: 4, y: 8, z: 8 (z_hi: 2, z_lo: 4; z = z_hi * 4 + z_lo), core: 2. Of those that a mesh axis runs over, the one named last changes fastest.
Arguments:
- orbitals: bfloat16 [2, 1024, 32, 4096], P(None, ('row', 'col'), 'depth'), may hold values from -20 to 20
- potential: float32 [32, 4096], P('depth'), may hold values from -6 to 6
Outputs:
- intersection: float32 [1024, 2, 1024], P(('row', 'depth'), None, 'col')
- applied: bfloat16 [2, 1024, 32, 4096], P(None, ('row', 'col'), 'depth')
The draws below stay inside these ranges and needn't reach their ends.
All inputs are finite; a program needn't handle non-finite values.
Results may differ from the reference program's by a relative error of at most 0.001.
Values may be sent and summed in bfloat16 or wider, within the bound.
No kernel may reach another device: no remote copies, remote signals or barrier semaphores. Data moves between devices by JAX's collectives and lax.ppermute only.
A program may use at most 128 MiB of HBM per device.

```python
import jax
import jax.numpy as jnp
from jax import lax

NORB = 1024
NX = 64
NZ = 32
NYX = 4096


def draw_orbitals(key, part):
    base_key = jax.random.fold_in(key, 11)
    first, second = jax.random.split(base_key, 2)
    shape = (2, NORB, NZ, NYX)
    noise = jnp.clip(jax.random.normal(first, shape, jnp.float32), -4.0, 4.0)
    scales = jnp.exp(jax.random.uniform(second, (1, NORB, 1, 1), jnp.float32, -0.69, 0.69))
    mixed = noise + 0.6 * jnp.roll(noise, 1, axis=1) + 0.4 * jnp.roll(noise, 37, axis=1)
    total = mixed * scales
    return jnp.clip(total, -20.0, 20.0).astype(jnp.bfloat16)


def block_levels(own_key, dims, shards, low, largest):
    def one(axis_at, shards_of):
        draws = jax.random.uniform(jax.random.fold_in(jax.random.fold_in(own_key, 6), axis_at), (shards_of,), jnp.float32, low / len(shards), largest / len(shards))
        return jnp.repeat(jnp.exp(draws), dims[axis_at] // shards_of).reshape((-1,) + (1,) * (len(dims) - axis_at - 1))

    gain = one(*shards[0])
    for cut in shards[1:]:
        gain = gain * one(*cut)
    return gain


def gaussian(own_key, dims, deviation, bound, cuts=(), dtype=jnp.bfloat16):
    level = block_levels(own_key, dims, cuts, -0.22, 0.18) if cuts else 1.0
    array = jax.random.normal(own_key, dims, jnp.float32) * deviation * level
    return jnp.minimum(jnp.maximum(array, -bound), bound).astype(dtype)


def setup_inputs(seed: int = 0) -> dict:
    arg_keys = jax.random.split(jax.random.key(seed), 3)
    return {
        "orbitals": draw_orbitals(jax.random.fold_in(arg_keys[2], 71), 0),
        "potential": gaussian(arg_keys[1], (NZ, NYX), 1.0, 6.0, ((0, 32),), jnp.float32),
    }


def apply_operator(field, potential):
    flat_cells = field.shape[-1]
    xpos = jnp.arange(flat_cells) % NX
    below = jnp.roll(field, 1, axis=2)
    above = jnp.roll(field, -1, axis=2)
    yminus = jnp.roll(field, NX, axis=3)
    yplus = jnp.roll(field, -NX, axis=3)
    xminus = jnp.where(xpos == 0, jnp.roll(field, 1 - NX, axis=3), jnp.roll(field, 1, axis=3))
    xplus = jnp.where(xpos == NX - 1, jnp.roll(field, NX - 1, axis=3), jnp.roll(field, -1, axis=3))
    lap = below + above + yminus + yplus + xminus + xplus - 6.0 * field
    return -0.5 * lap + potential[None, None] * field


def reference(orbitals, potential):
    wide = orbitals.astype(jnp.float32)
    cells = NZ * NYX
    real_part = wide[0].reshape(NORB, cells)
    imag_part = wide[1].reshape(NORB, cells)
    dvol = 1.0 / cells
    high = lax.Precision.HIGHEST
    sreal = jnp.dot(real_part, real_part.T, precision=high) + jnp.dot(imag_part, imag_part.T, precision=high)
    simag = jnp.dot(real_part, imag_part.T, precision=high) - jnp.dot(imag_part, real_part.T, precision=high)
    intersection = jnp.stack([sreal * dvol, simag * dvol], axis=1)
    applied = apply_operator(wide, potential).astype(jnp.bfloat16)
    return intersection, applied
```

```python
import functools

import jax
import jax.numpy as jnp
from jax import lax
from jax.experimental import pallas as pl
from jax.experimental.pallas import tpu as pltpu
from jax.sharding import Mesh
from jax.sharding import PartitionSpec as P

NX = 64
ORB = 64
CELLS = 4096
BLOCK = 1024
RING = ("zl", "y", "zh", "core")
ALL = ("x", "zl", "y", "zh", "core")


def ring_index(z, y, core):
    return ((z % 4) * 8 + y) * 4 + (z // 4) * 2 + core


def hop_table(last):
    pairs = []
    for z in range(8):
        for y in range(8):
            for core in range(2):
                step = 1 if core else -1
                to_z, to_y, to_core = (z + step) % 8, y, core
                if last:
                    start_hi = ((z - 3 * step) % 8) // 4
                    to_core = 1 - core
                    if core and start_hi == 1:
                        to_y = (y + 1) % 8
                    if not core and start_hi == 0:
                        to_y = (y - 1) % 8
                pairs.append((ring_index(z, y, core), ring_index(to_z, to_y, to_core)))
    return pairs


def turn_table(flip):
    pairs = []
    for x in range(4):
        for zl in range(4):
            for y in range(8):
                for zh in range(2):
                    for core in range(2):
                        a, h = y // 2, y % 2
                        source = ((x * 4 + zl) * 8 + y) * 4 + zh * 2 + core
                        to_y = zl * 2 + h
                        target = ((a * 4 + x) * 8 + to_y) * 4 + (zh ^ flip) * 2 + core
                        pairs.append((source, target))
    return pairs


def place():
    return lax.axis_index("x"), lax.axis_index("zl"), lax.axis_index("core")


def gram_kernel(steps, last, scale, *refs):
    count = len(steps)
    panels = refs[: 2 * count]
    others = refs[2 * count : 2 * count + 8]
    rest = refs[2 * count + 8 :]
    if last:
        before, mine, send, acc, table, turned = rest
    else:
        table, acc = rest
    k = pl.program_id(0)
    left = jnp.concatenate([p[...].reshape(ORB, BLOCK) for p in panels], axis=0)
    right = jnp.concatenate([o[...].reshape(ORB, BLOCK) for o in others], axis=0)
    part = lax.dot_general(
        left, right, (((1,), (1,)), ((), ())), preferred_element_type=jnp.float32
    )

    @pl.when(k == 0)
    def _():
        acc[...] = part

    @pl.when(k > 0)
    def _():
        acc[...] += part

    @pl.when(k == pl.num_programs(0) - 1)
    def _():
        x, zl, core = place()
        if last:
            table[...] = before[...]
        sign = jnp.where(lax.broadcasted_iota(jnp.int32, (ORB, 128), 1) < 64, 1.0, -1.0)
        for at, step in enumerate(steps):
            row = lax.rem(jnp.where(core == 1, zl + 4 - step, zl + step), 4)
            reach = jnp.where(core == 1, zl, 3 - zl)
            weight = jnp.where(reach >= step, 0.5 * scale if step == 0 else scale, 0.0)
            for other in range(4):
                col = lax.rem(x + other, 4)
                top = acc[at * 128 : at * 128 + 64, other * 128 : other * 128 + 128]
                low = acc[at * 128 + 64 : at * 128 + 128, other * 128 : other * 128 + 128]
                tile = (top + sign * pltpu.roll(low, 64, 1)) * weight
                table[col, pl.ds(pl.multiple_of(row * 64, 64), 64), :] = tile
        if last:
            for col in range(4):
                flipped = table[col].T
                turned[col, 0:64] = flipped[0:64]
                turned[col, 64:128] = -flipped[64:128]
            for out, which in ((mine, core), (send, 1 - core)):
                for y in range(8):
                    for zh in range(2):
                        base = y * 32 + zh * 16
                        rows = pl.ds(pl.multiple_of(base + which * 8, 8), 8)
                        for col in range(4):
                            at = (col * 2 + zh) * 8
                            out[y, at : at + 8, :] = table[col, rows, :]
                        for p in range(2):
                            base = p * 64 + (y % 2) * 32 + zh * 16
                            rows = pl.ds(pl.multiple_of(base + which * 8, 8), 8)
                            for half in range(2):
                                at = 64 + ((zh * 2 + p) * 2 + half) * 8
                                out[y, at : at + 8, :] = turned[
                                    y // 2, rows, half * 128 : half * 128 + 128
                                ]


def gram(steps, panels, others, scale, before=None):
    last = before is not None
    count = len(steps)

    def spec(a, part):
        if a.ndim == 2:
            return pl.BlockSpec((ORB, BLOCK), lambda k: (0, k))
        return pl.BlockSpec((1, ORB, BLOCK), lambda k: (part, 0, k))

    whole = lambda shape: pl.BlockSpec(shape, lambda k: (0,) * len(shape))
    operands, specs = [], []
    for re, im in panels + others:
        operands += [re, im]
        specs += [spec(re, 0), spec(im, 1)]
    acc = pltpu.VMEM((count * 128, 512), jnp.float32)
    table = (4, 256, 128)
    if last:
        operands.append(before)
        specs.append(whole(table))
        share = (8, 128, 128)
        out_shape = [jax.ShapeDtypeStruct(share, jnp.float32)] * 2
        out_specs = [whole(share)] * 2
        scratch = [acc, pltpu.VMEM(table, jnp.float32), pltpu.VMEM((4, 128, 256), jnp.float32)]
    else:
        out_shape = jax.ShapeDtypeStruct(table, jnp.float32)
        out_specs = whole(table)
        scratch = [acc]
    return pl.pallas_call(
        functools.partial(gram_kernel, steps, last, scale),
        grid=(CELLS // BLOCK,),
        in_specs=specs,
        out_specs=out_specs,
        out_shape=out_shape,
        scratch_shapes=scratch,
        compiler_params=pltpu.CompilerParams(dimension_semantics=("arbitrary",)),
        name="gram_last" if last else "gram_first",
    )(*operands)


def apply_kernel(own, near, far_re, far_im, potential, out):
    part = pl.program_id(0)
    center = own[...].reshape(-1, CELLS).astype(jnp.float32)
    near_value = near[...].reshape(-1, CELLS).astype(jnp.float32)
    far = jnp.where(part == 0, far_re[...], far_im[...])
    rows = center.shape[0]
    lane = lax.broadcasted_iota(jnp.int32, (rows, 128), 1)
    first, final = lane % NX == 0, lane % NX == NX - 1
    low = lane < NX
    tiles = [center[:, c * 128 : c * 128 + 128] for c in range(CELLS // 128)]
    swapped = [pltpu.roll(t, NX, 1) for t in tiles]
    count = len(tiles)
    for c, t in enumerate(tiles):
        span = slice(c * 128, c * 128 + 128)
        y_minus = jnp.where(low, swapped[(c - 1) % count], swapped[c])
        y_plus = jnp.where(low, swapped[c], swapped[(c + 1) % count])
        x_minus = jnp.where(first, pltpu.roll(t, 128 - (NX - 1), 1), pltpu.roll(t, 1, 1))
        x_plus = jnp.where(final, pltpu.roll(t, NX - 1, 1), pltpu.roll(t, 127, 1))
        lap = near_value[:, span] + far[:, span].astype(jnp.float32)
        lap = lap + y_minus + y_plus + x_minus + x_plus - 6.0 * t
        value = -0.5 * lap + potential[:, span] * t
        out[0, :, span] = value.astype(jnp.bfloat16)


def apply_operator(own, near, far_re, far_im, potential):
    rows = 16
    both = pl.BlockSpec((1, rows, CELLS), lambda p, r: (p, r, 0))
    return pl.pallas_call(
        apply_kernel,
        grid=(2, ORB // rows),
        in_specs=[
            both,
            both,
            pl.BlockSpec((rows, CELLS), lambda p, r: (jnp.where(p == 0, r, ORB // rows - 1), 0)),
            pl.BlockSpec((rows, CELLS), lambda p, r: (jnp.where(p == 1, r, 0), 0)),
            pl.BlockSpec((1, CELLS), lambda p, r: (0, 0)),
        ],
        out_specs=both,
        out_shape=jax.ShapeDtypeStruct(own.shape, jnp.bfloat16),
        name="apply",
    )(own, near, far_re, far_im, potential)


def shards(orbitals, potential):
    parts, orbs, planes, cells = orbitals.shape
    own = orbitals.reshape(parts, orbs, cells)
    scale = 1.0 / (32 * cells)
    up = [(i, (i + 1) % 4) for i in range(4)]
    down = [(i, (i - 1) % 4) for i in range(4)]

    from_low = lax.ppermute(own, "x", up)
    from_high = lax.ppermute(own, "x", down)
    re, im = own[0], own[1]
    panels = [(own, own)]
    for hop in range(4):
        table = hop_table(hop == 3)
        re, im = lax.ppermute(re, RING, table), lax.ppermute(im, RING, table)
        panels.append((re, im))
    near = lax.ppermute(own, "core", [(0, 1), (1, 0)])
    far_re = lax.ppermute(from_low[0], "x", up)
    far_im = lax.ppermute(from_high[1], "x", down)
    others = [(own, own), (from_high, from_high), (far_re, far_im), (from_low, from_low)]

    table = gram((0, 1, 2), panels[:3], others, scale)
    mine, send = gram((3,), panels[3:4], others, scale, table)
    share = mine + lax.ppermute(send, "core", [(0, 1), (1, 0)])
    pieces = lax.all_to_all(share, "y", 0, 0, tiled=True)
    total = jnp.sum(pieces, axis=0)

    direct = total[:64].reshape(8, 8, 128)
    direct = lax.all_to_all(direct, ("zl", "zh"), 0, 0, tiled=True)
    direct = direct.reshape(4, 2, 8, 2, 64).sum(axis=1)
    direct = direct.transpose(1, 2, 0, 3).reshape(8, 2, 256)
    turned = total[64:].reshape(2, 32, 128)
    zh = lax.axis_index("zh")
    keep = lax.dynamic_index_in_dim(turned, zh, 0, False)
    give = lax.dynamic_index_in_dim(turned, 1 - zh, 0, False)
    turned = lax.ppermute(keep, ALL, turn_table(0)) + lax.ppermute(give, ALL, turn_table(1))
    turned = turned.reshape(2, 2, 8, 128).transpose(2, 0, 1, 3).reshape(8, 2, 256)

    applied = apply_operator(own, near, *panels[4], potential)
    return direct + turned, applied.reshape(orbitals.shape)


def solution(mesh):
    fine = Mesh(mesh.devices.reshape(4, 4, 8, 2, 2), ALL)
    depth = ("y", "zh", "core")
    in_specs = (P(None, ("x", "zl"), depth, None), P(depth, None))
    out_specs = (P(("x",) + depth, None, "zl"), P(None, ("x", "zl"), depth, None))
    return jax.shard_map(shards, mesh=fine, in_specs=in_specs, out_specs=out_specs, check_vma=False)
```
